32 devices in a mesh: seq: 8 (over z, y), mp: 4 (over x, core).
Axes of the slice: x: 2, y: 2, z: 4, core: 2. Of those that a mesh axis runs over, the one named last changes fastest.
Arguments:
- resid: bfloat16 [2048, 5120], P('seq', 'mp'), may hold values from -15 to 15
- queries: bfloat16 [2048, 5120], P('seq', 'mp'), may hold values from -28 to 28
- keys: bfloat16 [2048, 5120], P('seq', 'mp'), may hold values from -12.25 to 12.25
- values: bfloat16 [2048, 5120], P('seq', 'mp'), may hold values from -6 to 6
- doc_ids: int32 [2048], P('seq'), may hold values from 0 to 3, as said below
- out_proj: bfloat16 [5120, 5120], P('mp'), may hold values from -0.5 to 0.5
- ffn_gain: bfloat16 [5120], P('mp'), may hold values from 0.25 to 1.75
- w_in: bfloat16 [5120, 13824], P('mp', 'seq'), may hold values from -0.078125 to 0.078125
- w_out: bfloat16 [13824, 5120], P('seq', 'mp'), may hold values from -0.109375 to 0.109375
- hot_index: int32 [8, 384], P('seq'), may hold values from 0 to 1727, as said below
- hot_blocks: int32 [8], P('seq'), may hold values from 1 to 3, as said below
Outputs:
- layer_out: bfloat16 [2048, 5120], P('seq', 'mp')
- hot_mean: float32 [8, 384], P('seq')
The draws below stay inside these ranges and needn't reach their ends.
Inputs may be any that keep to these rules, and one draw needn't show every extreme that they name: `doc_ids`: document numbers never fall along the tokens; every number from 0 to 3 occurs; some document has 1024 tokens. `hot_index`: row g holds 384 distinct neuron numbers of group g; only its first 128 * hot_blocks[g] entries are live, the others are ignored. `hot_blocks`: some group has exactly 3 live blocks.
All inputs are finite; a program needn't handle non-finite values.
Results may differ from the reference program's by a relative error of at most 0.014.
Values may be sent and summed in bfloat16 or wider, within the bound.
A program may use at most 192 MiB of HBM per device.

```python
import jax
import jax.numpy as jnp
from jax import lax

D = 5120
HEADS = 40
HEAD_DIM = 128
FF = 13824
BLOCK = 128
CAP = 3
TOKENS = 2048
GROUPS = 8
NEURONS = 1728
SLOTS = 384


def paired_rows(key, which):
    noise = jnp.clip(jax.random.normal(jax.random.fold_in(key, 101 + which), (TOKENS, D), jnp.float32), -4.0, 4.0)
    return noise


def draw_resid(key, part):
    ramp = jnp.arange(D, dtype=jnp.float32) / (D - 1)
    rough = jnp.exp(jax.random.uniform(jax.random.fold_in(key, 501), (D,), jnp.float32, jnp.log(0.7), jnp.log(1.4)))
    column_scale = 0.5 * jnp.exp(ramp * jnp.log(5.0)) * rough
    noise = jnp.clip(jax.random.normal(jax.random.fold_in(key, 504), (TOKENS, D), jnp.float32), -4.0, 4.0)
    return (noise * column_scale[None, :]).astype(jnp.bfloat16)


def draw_queries(key, part):
    return paired_rows(key, 0).astype(jnp.bfloat16)


def draw_keys(key, part):
    return paired_rows(key, 1).astype(jnp.bfloat16)


def draw_doc_ids(key, part):
    half = TOKENS // 2
    cut_one = jax.random.randint(jax.random.fold_in(key, 401), (), 1, half - 1)
    cut_two = cut_one + half
    cut_three = jax.random.randint(jax.random.fold_in(key, 402), (), cut_two + 1, TOKENS)
    places = jnp.arange(TOKENS, dtype=jnp.int32)
    marks = (places >= cut_one).astype(jnp.int32) + (places >= cut_two).astype(jnp.int32) + (places >= cut_three).astype(jnp.int32)
    return marks.astype(jnp.int32)


def draw_hot_index(key, part):
    group_keys = jax.random.split(jax.random.fold_in(key, 201), GROUPS)
    orders = jax.vmap(lambda single: jax.random.permutation(single, NEURONS))(group_keys)
    return orders[:, :SLOTS].astype(jnp.int32)


def draw_hot_blocks(key, part):
    busy = jax.random.randint(jax.random.fold_in(key, 301), (GROUPS,), 0, 3) == 0
    extra = jax.random.randint(jax.random.fold_in(key, 302), (GROUPS,), 2, CAP + 1)
    counts = jnp.where(busy, extra, 1)
    heaviest = jax.random.randint(jax.random.fold_in(key, 303), (), 0, GROUPS)
    return jnp.where(jnp.arange(GROUPS) == heaviest, CAP, counts).astype(jnp.int32)


def block_levels(stream_key, shape, cuts, least, largest):
    level = 1.0
    for position, parts in cuts:
        steps = jax.random.uniform(jax.random.fold_in(jax.random.fold_in(stream_key, 6), position), (parts,), jnp.float32, least / len(cuts), largest / len(cuts))
        level = level * jnp.repeat(jnp.exp(steps), shape[position] // parts).reshape((-1,) + (1,) * (len(shape) - 1 - position))
    return level


def bell_draw(stream_key, shape, deviation, bound, shards=(), kind=jnp.bfloat16):
    factor_of = block_levels(stream_key, shape, shards, -0.22, 0.18) if shards else 1.0
    values = jax.random.normal(stream_key, shape, jnp.float32) * deviation * factor_of
    return jnp.minimum(jnp.maximum(values, -bound), bound).astype(kind)


def setup_inputs(seed: int = 0) -> dict:
    splits = jax.random.split(jax.random.key(seed), 12)
    return {
        "resid": draw_resid(jax.random.fold_in(splits[11], 71), 0),
        "queries": draw_queries(jax.random.fold_in(splits[11], 71), 0),
        "keys": draw_keys(jax.random.fold_in(splits[11], 71), 0),
        "values": bell_draw(splits[3], (TOKENS, D), 1.0, 6.0, ((0, 8), (1, 4))),
        "doc_ids": draw_doc_ids(jax.random.fold_in(splits[11], 71), 0),
        "out_proj": bell_draw(splits[5], (D, D), HEAD_DIM ** -0.5, 0.5, ((0, 4),)),
        "ffn_gain": jnp.clip(1.0 + 0.15 * jax.random.normal(splits[6], (D,), jnp.float32), 0.25, 1.75).astype(jnp.bfloat16),
        "w_in": bell_draw(splits[7], (D, FF), D ** -0.5, 0.078125, ((0, 4), (1, 8))),
        "w_out": bell_draw(splits[8], (FF, D), (FF // 4) ** -0.5, 0.109375, ((0, 8), (1, 4))),
        "hot_index": draw_hot_index(jax.random.fold_in(splits[11], 71), 0),
        "hot_blocks": draw_hot_blocks(jax.random.fold_in(splits[11], 71), 0),
    }


epsilon = 1e-05
masked_score = -1e+30

def reference(resid, queries, keys, values, doc_ids, out_proj, ffn_gain, w_in, w_out, hot_index, hot_blocks):
    scale = HEAD_DIM ** (-0.5)
    positions = jnp.arange(TOKENS, dtype=jnp.int32)
    visible = (positions[:, None] >= positions[None, :]) & (doc_ids[:, None] == doc_ids[None, :])

    def one_head(triple):
        query_head, key_head, value_head = triple
        scores = jnp.dot(query_head, key_head.T, preferred_element_type=jnp.float32) * scale
        scores = jnp.where(visible, scores, masked_score)
        top = lax.optimization_barrier(jnp.max(scores, axis=1, keepdims=True))
        weights = jnp.where(visible, jnp.exp(scores - top), 0.0)
        total = lax.optimization_barrier(jnp.sum(weights, axis=1, keepdims=True))
        mixed = jnp.dot(weights.astype(jnp.bfloat16), value_head, preferred_element_type=jnp.float32)
        return (mixed / total).astype(jnp.bfloat16)
    split_queries = queries.reshape(TOKENS, HEADS, HEAD_DIM).transpose(1, 0, 2)
    split_keys = keys.reshape(TOKENS, HEADS, HEAD_DIM).transpose(1, 0, 2)
    split_values = values.reshape(TOKENS, HEADS, HEAD_DIM).transpose(1, 0, 2)
    attended = lax.map(one_head, (split_queries, split_keys, split_values))
    attended = attended.transpose(1, 0, 2).reshape(TOKENS, D)
    projected = jnp.dot(attended, out_proj, preferred_element_type=jnp.float32)
    state_rows = (resid.astype(jnp.float32) + projected).astype(jnp.bfloat16)
    widened = state_rows.astype(jnp.float32)
    inverse = lax.rsqrt(lax.optimization_barrier(jnp.mean(widened * widened, axis=1, keepdims=True)) + epsilon)
    normed = (widened * inverse * ffn_gain.astype(jnp.float32)).astype(jnp.bfloat16)
    slot_ids = jnp.arange(SLOTS, dtype=jnp.int32)

    def one_group(carry, group):
        columns = (group * NEURONS + hot_index[group]).astype(jnp.int32)
        live = slot_ids < BLOCK * hot_blocks[group]
        before = jnp.dot(normed, jnp.take(w_in, columns, axis=1), preferred_element_type=jnp.float32)
        active = jnp.where(live[None, :], jnp.maximum(before, 0.0), 0.0)
        carry = carry + jnp.dot(active.astype(jnp.bfloat16), jnp.take(w_out, columns, axis=0), preferred_element_type=jnp.float32)
        return (carry, lax.optimization_barrier(jnp.mean(active, axis=0)))
    ffn_sum, hot_mean = lax.scan(one_group, jnp.zeros((TOKENS, D), jnp.float32), jnp.arange(GROUPS, dtype=jnp.int32))
    layer_out = (widened + ffn_sum).astype(jnp.bfloat16)
    return (layer_out, hot_mean)
```

```python
import functools

import jax
import jax.numpy as jnp
from jax import lax
from jax.experimental import pallas as pl
from jax.experimental.pallas import tpu as pltpu
from jax.sharding import PartitionSpec as P

HEAD_DIM = 128
BLOCK = 128
MESH = pl.DeviceIdType.MESH
VMEM = pltpu.VMEM

epsilon = 1e-05
masked_score = -1e30


def row_length(mesh):
    seq = mesh.shape["seq"]
    try:
        first = [mesh.devices[i, 0].coords for i in range(seq)]
        size = len({c[1] for c in first})
        if seq % size == 0:
            return size
    except (AttributeError, IndexError, TypeError):
        pass
    return 2


def gather_kernel(nz, ny, up, down, window, chunks, count, *refs):
    ins = refs[:count]
    outs = refs[count : 2 * count]
    sems = refs[2 * count :]
    own_sem, zs_sem, zr_sem, ys_sem, yr_sem = sems
    me = lax.axis_index("seq")
    mp = lax.axis_index("mp")
    z = me // ny
    y = me % ny

    def dev(zz, yy):
        return (zz * ny + yy, mp)

    barrier = pltpu.get_barrier_semaphore()
    for step in (-1, 1):
        ok = (z + step >= 0) & (z + step < nz)

        @pl.when(ok)
        def _(step=step):
            pl.semaphore_signal(barrier, inc=1, device_id=dev(z + step, y), device_id_type=MESH)

    for dy in range(1, ny):
        pl.semaphore_signal(
            barrier, inc=1, device_id=dev(z, (y + dy) % ny), device_id_type=MESH
        )
    below = jnp.where(z > 0, 1, 0)
    above = jnp.where(z < nz - 1, 1, 0)
    pl.semaphore_wait(barrier, below + above + ny - 1)

    def piece(ref, a, c):
        rows = ins[a].shape[0]
        if chunks[a] == 1:
            return ref
        size = rows // chunks[a]
        return ref.at[pl.ds(c * size, size)]

    def slot(a, zz, yy, c):
        return piece(outs[a].at[zz * ny + yy], a, c)

    base = []
    total = 0
    for a in range(count):
        base.append(total)
        total += chunks[a]

    def own_copy(a):
        return pltpu.make_async_copy(ins[a], outs[a].at[me], own_sem.at[a])

    def level_z(lv):
        return z - lv if lv <= up else z + (lv - up)

    def source(lv, a, c):
        if lv == 0:
            return piece(ins[a], a, c)
        return slot(a, level_z(lv), y, c)

    def z_copy(lv, direction, a, c):
        there = (lv + 1) if direction > 0 else (up + 1 if lv == 0 else lv + 1)
        return pltpu.make_async_remote_copy(
            src_ref=source(lv, a, c),
            dst_ref=slot(a, level_z(lv), y, c),
            send_sem=zs_sem.at[there - 1, base[a] + c],
            recv_sem=zr_sem.at[there - 1, base[a] + c],
            device_id=dev(z + direction, y),
            device_id_type=MESH,
        )

    def z_cond(lv, direction):
        src = level_z(lv)
        return (src >= 0) & (src < nz) & (z + direction >= 0) & (z + direction < nz)

    def y_needed(lv, y_from, y_to):
        src = level_z(lv)
        ok = (src >= 0) & (src < nz)
        if window is not None:
            offset = (z - src) * ny + y_to - y_from
            ok = ok & (offset >= 0) & (offset <= window)
        return ok

    def y_copy(lv, dy, a, c):
        return pltpu.make_async_remote_copy(
            src_ref=source(lv, a, c),
            dst_ref=slot(a, level_z(lv), y, c),
            send_sem=ys_sem.at[lv * (ny - 1) + dy - 1, base[a] + c],
            recv_sem=yr_sem.at[lv * (ny - 1) + dy - 1, base[a] + c],
            device_id=dev(z, (y + dy) % ny),
            device_id_type=MESH,
        )

    def y_arrival(lv, dy, a, c):
        return pltpu.make_async_remote_copy(
            src_ref=source(lv, a, c),
            dst_ref=slot(a, level_z(lv), (y + ny - dy) % ny, c),
            send_sem=ys_sem.at[lv * (ny - 1) + dy - 1, base[a] + c],
            recv_sem=yr_sem.at[lv * (ny - 1) + dy - 1, base[a] + c],
            device_id=dev(z, (y + dy) % ny),
            device_id_type=MESH,
        )

    every = [(a, c) for a in range(count) for c in range(chunks[a])]

    def directions(lv):
        out = []
        if lv < up:
            out.append(1)
        if down and (lv == 0 or (lv > up and lv - up < down)):
            out.append(-1)
        return out

    def spread(lv, a, c):
        for direction in directions(lv):

            @pl.when(z_cond(lv, direction))
            def _(direction=direction):
                z_copy(lv, direction, a, c).start()

        for dy in range(1, ny):

            @pl.when(y_needed(lv, y, (y + dy) % ny))
            def _(dy=dy):
                y_copy(lv, dy, a, c).start()

    for a, c in every:
        spread(0, a, c)
    for a in range(count):
        own_copy(a).start()
    order = []
    for k in range(1, max(up, down) + 1):
        for a, c in every:
            if k <= up:
                order.append((k, a, c))
            if k <= down:
                order.append((up + k, a, c))
    for lv, a, c in order:
        src = level_z(lv)

        @pl.when((src >= 0) & (src < nz))
        def _(lv=lv, a=a, c=c):
            pltpu.make_async_remote_copy(
                src_ref=slot(a, level_z(lv), y, c),
                dst_ref=slot(a, level_z(lv), y, c),
                send_sem=zs_sem.at[lv - 1, base[a] + c],
                recv_sem=zr_sem.at[lv - 1, base[a] + c],
                device_id=dev(z, (y + 1) % ny),
                device_id_type=MESH,
            ).wait_recv()
            spread(lv, a, c)

    for lv in range(up + down + 1):
        for a, c in every:
            for dy in range(1, ny):

                @pl.when(y_needed(lv, (y + ny - dy) % ny, y))
                def _(lv=lv, a=a, c=c, dy=dy):
                    y_arrival(lv, dy, a, c).wait_recv()

    for lv in range(up + down + 1):
        for a, c in every:
            for direction in directions(lv):

                @pl.when(z_cond(lv, direction))
                def _(lv=lv, a=a, c=c, direction=direction):
                    z_copy(lv, direction, a, c).wait_send()

            for dy in range(1, ny):

                @pl.when(y_needed(lv, y, (y + dy) % ny))
                def _(lv=lv, a=a, c=c, dy=dy):
                    y_copy(lv, dy, a, c).wait_send()

    for a in range(count):
        own_copy(a).wait()


def seq_gather(arrays, ny, causal, chunks, collective_id):
    n = lax.axis_size("seq")
    nz = n // ny
    if causal:
        window = n // 2
        up, down = min(nz - 1, -(-window // ny)), 0
    else:
        window = None
        up = down = nz - 1
    count = len(arrays)
    total = sum(chunks)
    levels = up + down
    return pl.pallas_call(
        functools.partial(gather_kernel, nz, ny, up, down, window, chunks, count),
        out_shape=[jax.ShapeDtypeStruct((n,) + a.shape, a.dtype) for a in arrays],
        in_specs=[pl.BlockSpec(memory_space=VMEM)] * count,
        out_specs=[pl.BlockSpec(memory_space=pl.ANY)] * count,
        scratch_shapes=[
            pltpu.SemaphoreType.DMA((count,)),
            pltpu.SemaphoreType.DMA((levels, total)),
            pltpu.SemaphoreType.DMA((levels, total)),
            pltpu.SemaphoreType.DMA(((levels + 1) * (ny - 1), total)),
            pltpu.SemaphoreType.DMA(((levels + 1) * (ny - 1), total)),
        ],
        compiler_params=pltpu.CompilerParams(
            collective_id=collective_id, has_side_effects=True
        ),
    )(*arrays)


def attention_kernel(window, scale, q_ref, k_ref, v_ref, qdoc_ref, kdoc_ref, out_ref):
    here = lax.axis_index("seq")
    rows = q_ref.shape[0]
    query = q_ref[...]
    query_doc = qdoc_ref[...]
    row = lax.broadcasted_iota(jnp.int32, (rows, rows), 0)
    col = lax.broadcasted_iota(jnp.int32, (rows, rows), 1)
    first = jnp.maximum(here - window, 0)

    def visit(block, carry):
        top, total, accum = carry
        scores = (
            lax.dot_general(
                query,
                k_ref[block],
                (((1,), (1,)), ((), ())),
                preferred_element_type=jnp.float32,
            )
            * scale
        )
        visible = (query_doc == kdoc_ref[block, 0:1, :]) & (
            row - col >= (block - here) * rows
        )
        scores = jnp.where(visible, scores, masked_score)
        new_top = jnp.maximum(top, jnp.max(scores, axis=1, keepdims=True))
        weights = jnp.where(visible, jnp.exp(scores - new_top), 0.0)
        fade = jnp.exp(top - new_top)
        total = total * fade + jnp.sum(weights, axis=1, keepdims=True)
        accum = accum * fade + jnp.dot(
            weights.astype(jnp.bfloat16), v_ref[block], preferred_element_type=jnp.float32
        )
        return new_top, total, accum

    start = (
        jnp.full((rows, 1), masked_score, jnp.float32),
        jnp.zeros((rows, 1), jnp.float32),
        jnp.zeros((rows, HEAD_DIM), jnp.float32),
    )
    _, total, accum = lax.fori_loop(first, here + 1, visit, start)
    out_ref[...] = (accum / total).astype(jnp.bfloat16)


def attention(queries, keys, values, doc_col, doc_rows):
    rows, width = queries.shape
    n = keys.shape[0]
    heads = width // HEAD_DIM
    return pl.pallas_call(
        functools.partial(attention_kernel, n // 2, HEAD_DIM ** (-0.5)),
        grid=(heads,),
        out_shape=jax.ShapeDtypeStruct((rows, width), jnp.bfloat16),
        in_specs=[
            pl.BlockSpec((rows, HEAD_DIM), lambda h: (0, h)),
            pl.BlockSpec((n, rows, HEAD_DIM), lambda h: (0, 0, h)),
            pl.BlockSpec((n, rows, HEAD_DIM), lambda h: (0, 0, h)),
            pl.BlockSpec((rows, 1), lambda h: (0, 0)),
            pl.BlockSpec(doc_rows.shape, lambda h: (0, 0, 0)),
        ],
        out_specs=pl.BlockSpec((rows, HEAD_DIM), lambda h: (0, h)),
    )(queries, keys, values, doc_col, doc_rows)


def mp_scatter_kernel(n, x_ref, out_ref, near, sums, far, s1, r1, s2, r2):
    seq = lax.axis_index("seq")
    me = lax.axis_index("mp")
    chips = n // 2
    chip = me // 2
    core = me % 2
    partner = chip * 2 + 1 - core
    width = out_ref.shape[1]
    barrier = pltpu.get_barrier_semaphore()
    pl.semaphore_signal(barrier, inc=1, device_id=(seq, partner), device_id_type=MESH)
    for d in range(1, chips):
        other = ((chip + d) % chips) * 2 + core
        pl.semaphore_signal(barrier, inc=1, device_id=(seq, other), device_id_type=MESH)
    pl.semaphore_wait(barrier, chips)

    def columns(index):
        return pl.ds(pl.multiple_of(index * width, 128), width)

    first = []
    for d in list(range(1, chips)) + [0]:
        target = (chip + d) % chips
        copy = pltpu.make_async_remote_copy(
            src_ref=x_ref.at[:, columns(target * 2 + 1 - core)],
            dst_ref=near.at[d],
            send_sem=s1.at[d],
            recv_sem=r1.at[d],
            device_id=(seq, partner),
            device_id_type=MESH,
        )
        copy.start()
        first.append((d, target, copy))
    second = []
    for d, target, copy in first:
        copy.wait_recv()
        mine = x_ref[:, columns(target * 2 + core)].astype(jnp.float32)
        total = mine + near[d].astype(jnp.float32)
        if d == 0:
            out_ref[...] = total
            continue
        sums[d - 1] = total.astype(jnp.bfloat16)
        send = pltpu.make_async_remote_copy(
            src_ref=sums.at[d - 1],
            dst_ref=far.at[d - 1],
            send_sem=s2.at[d - 1],
            recv_sem=r2.at[d - 1],
            device_id=(seq, target * 2 + core),
            device_id_type=MESH,
        )
        send.start()
        second.append((d, send))
    for d, send in second:
        send.wait_recv()
        out_ref[...] += far[d - 1].astype(jnp.float32)
    for d, target, copy in first:
        copy.wait_send()
    for d, send in second:
        send.wait_send()


def mp_scatter(x, collective_id):
    n = lax.axis_size("mp")
    rows, total = x.shape
    width = total // n
    chips = n // 2
    return pl.pallas_call(
        functools.partial(mp_scatter_kernel, n),
        out_shape=jax.ShapeDtypeStruct((rows, width), jnp.float32),
        in_specs=[pl.BlockSpec(memory_space=VMEM)],
        out_specs=pl.BlockSpec(memory_space=VMEM),
        scratch_shapes=[
            VMEM((chips, rows, width), jnp.bfloat16),
            VMEM((chips - 1, rows, width), jnp.bfloat16),
            VMEM((chips - 1, rows, width), jnp.bfloat16),
            pltpu.SemaphoreType.DMA((chips,)),
            pltpu.SemaphoreType.DMA((chips,)),
            pltpu.SemaphoreType.DMA((chips - 1,)),
            pltpu.SemaphoreType.DMA((chips - 1,)),
        ],
        compiler_params=pltpu.CompilerParams(
            collective_id=collective_id, has_side_effects=True, vmem_limit_bytes=48 * 1024 * 1024
        ),
    )(x)


def seq_scatter_kernel(nz, ny, x_ref, out_ref, near, sums, far, s1, r1, s2, r2):
    me = lax.axis_index("seq")
    mp = lax.axis_index("mp")
    z = me // ny
    y = me % ny
    barrier = pltpu.get_barrier_semaphore()
    for d in range(1, ny):
        peer = z * ny + (y + d) % ny
        pl.semaphore_signal(barrier, inc=1, device_id=(peer, mp), device_id_type=MESH)
    for d in range(1, nz):
        peer = ((z + d) % nz) * ny + y
        pl.semaphore_signal(barrier, inc=1, device_id=(peer, mp), device_id_type=MESH)
    pl.semaphore_wait(barrier, ny + nz - 2)

    first = []
    for d in list(range(1, nz)) + [0]:
        target = (z + d) % nz
        group = []
        for e in range(1, ny):
            other = (y + e) % ny
            copy = pltpu.make_async_remote_copy(
                src_ref=x_ref.at[target * ny + other],
                dst_ref=near.at[d, e - 1],
                send_sem=s1.at[d, e - 1],
                recv_sem=r1.at[d, e - 1],
                device_id=(z * ny + other, mp),
                device_id_type=MESH,
            )
            copy.start()
            group.append(copy)
        first.append((d, target, group))
    second = []
    for d, target, group in first:
        total = x_ref[target * ny + y].astype(jnp.float32)
        for e, copy in enumerate(group):
            copy.wait_recv()
            total = total + near[d, e].astype(jnp.float32)
        if d == 0:
            out_ref[...] = total
            continue
        sums[d - 1] = total.astype(jnp.bfloat16)
        send = pltpu.make_async_remote_copy(
            src_ref=sums.at[d - 1],
            dst_ref=far.at[d - 1],
            send_sem=s2.at[d - 1],
            recv_sem=r2.at[d - 1],
            device_id=(target * ny + y, mp),
            device_id_type=MESH,
        )
        send.start()
        second.append((d, send))
    for d, send in second:
        send.wait_recv()
        out_ref[...] += far[d - 1].astype(jnp.float32)
    for d, target, group in first:
        for copy in group:
            copy.wait_send()
    for d, send in second:
        send.wait_send()


def seq_scatter(x, ny, collective_id):
    n, rows, width = x.shape
    nz = n // ny
    dma = pltpu.SemaphoreType.DMA
    return pl.pallas_call(
        functools.partial(seq_scatter_kernel, nz, ny),
        out_shape=jax.ShapeDtypeStruct((rows, width), jnp.float32),
        in_specs=[pl.BlockSpec(memory_space=VMEM)],
        out_specs=pl.BlockSpec(memory_space=VMEM),
        scratch_shapes=[
            VMEM((nz, ny - 1, rows, width), jnp.bfloat16),
            VMEM((nz - 1, rows, width), jnp.bfloat16),
            VMEM((nz - 1, rows, width), jnp.bfloat16),
            dma((nz, ny - 1)),
            dma((nz, ny - 1)),
            dma((nz - 1,)),
            dma((nz - 1,)),
        ],
        compiler_params=pltpu.CompilerParams(
            collective_id=collective_id, has_side_effects=True, vmem_limit_bytes=48 * 1024 * 1024
        ),
    )(x)


def reduce_pre(partial_pre, live):
    summed = lax.psum(partial_pre.astype(jnp.bfloat16), "mp").astype(jnp.float32)
    active = jnp.where(live[None, :], jnp.maximum(summed, 0.0), 0.0)
    column_sums = jnp.sum(active, axis=0)
    return (active.astype(jnp.bfloat16), column_sums)


def local(
    ny,
    resid,
    queries,
    keys,
    values,
    doc_ids,
    out_proj,
    ffn_gain,
    w_in,
    w_out,
    hot_index,
    hot_blocks,
):
    tok_dev, width_dev = resid.shape
    groups = lax.axis_size("seq")
    width = width_dev * lax.axis_size("mp")
    total_tokens = tok_dev * groups
    doc_row = jnp.broadcast_to(doc_ids[None, :], (8, tok_dev))
    doc_rows, all_keys, all_values = seq_gather(
        [doc_row, keys, values], ny, True, (1, 2, 2), 0
    )
    chosen = hot_index[0]
    slots = chosen.shape[0]
    hot_in = jnp.take(w_in, chosen, axis=1)
    hot_out = jnp.take(w_out, chosen, axis=0)
    live = jnp.arange(slots, dtype=jnp.int32) < BLOCK * hot_blocks[0]
    attended = attention(queries, all_keys, all_values, doc_ids[:, None], doc_rows)
    projected = jnp.dot(attended, out_proj, preferred_element_type=jnp.float32)
    projected = mp_scatter(projected.astype(jnp.bfloat16), 1)
    state_rows = (resid.astype(jnp.float32) + projected).astype(jnp.bfloat16)
    widened = state_rows.astype(jnp.float32)
    squares = lax.psum(jnp.sum(widened * widened, axis=1), "mp")
    inverse = lax.rsqrt(squares / width + epsilon)
    normed = (widened * inverse[:, None] * ffn_gain.astype(jnp.float32)).astype(jnp.bfloat16)
    (all_normed,) = seq_gather([normed], ny, False, (4,), 2)
    partial_pre = jnp.dot(
        all_normed.reshape(total_tokens, width_dev),
        hot_in,
        preferred_element_type=jnp.float32,
    )
    active_low, column_sums = reduce_pre(partial_pre, live)
    hot_mean = (column_sums / total_tokens)[None, :]
    contribution = jnp.dot(active_low, hot_out, preferred_element_type=jnp.float32)
    contribution = contribution.astype(jnp.bfloat16).reshape(groups, tok_dev, width_dev)
    ffn_out = seq_scatter(contribution, ny, 3)
    layer_out = (widened + ffn_out).astype(jnp.bfloat16)
    return (layer_out, hot_mean)


def solution(mesh):
    return jax.shard_map(
        functools.partial(local, row_length(mesh)),
        mesh=mesh,
        in_specs=(
            P("seq", "mp"),
            P("seq", "mp"),
            P("seq", "mp"),
            P("seq", "mp"),
            P("seq"),
            P("mp", None),
            P("mp"),
            P("mp", "seq"),
            P("seq", "mp"),
            P("seq", None),
            P("seq"),
        ),
        out_specs=(P("seq", "mp"), P("seq", None)),
        check_vma=False,
    )
```
